32 devices in a mesh: row: 4 (over y, x), col: 8 (over z, core).
Axes of the slice: x: 2, y: 2, z: 4, core: 2. Of those that a mesh axis runs over, the one named last changes fastest.
Arguments:
- activations: bfloat16 [1024, 9216], P('col', 'row'), may hold values from -64 to 64
- output_grads: bfloat16 [1024, 73728], P('row', 'col'), may hold values from -16 to 16
- weight: bfloat16 [9216, 73728], P('row', 'col'), may hold values from -1 to 1
- row_moment: float32 [9216], P('row'), may hold values from 0.01 to 0.3
- col_moment: float32 [73728], P('col'), may hold values from 0.01 to 0.3
Outputs:
- new_weight: bfloat16 [9216, 73728], P('row', 'col')
- new_row: float32 [9216], P('row')
- new_col: float32 [73728], P('col')
The draws below stay inside these ranges and needn't reach their ends.
All inputs are finite; a program needn't handle non-finite values.
Results may differ from the reference program's by a relative error of at most 0.0004.
Values may be sent and summed in bfloat16 or wider, within the bound.
No kernel may reach another device: no remote copies, remote signals or barrier semaphores. Data moves between devices by JAX's collectives and lax.ppermute only.
A program may use at most 256 MiB of HBM per device.

```python
import math
import jax
import jax.numpy as jnp
from jax import lax

D = 9216
FF = 73728
TOKENS = 1024


def scales(key, length, trend, spread):
    position = jnp.arange(length, dtype=jnp.float32) / length
    jitter = jax.random.uniform(key, (length,), jnp.float32, 0.0, math.log(spread))
    return jnp.exp(math.log(trend) * position + jitter)


def shaped_panel(key, rows_total, width, divisor):
    keys = jax.random.split(key, 2)
    values = jax.random.normal(keys[0], (rows_total, width), jnp.float32)
    factor = scales(keys[1], width, 3.0, 10.0) / 4.0
    return values * factor[None, :] / divisor


def draw_activations(key, part):
    values = shaped_panel(jax.random.fold_in(key, 11), TOKENS, D, 1.0)
    return jnp.clip(values, -64.0, 64.0).astype(jnp.bfloat16)


def draw_output_grads(key, part):
    values = shaped_panel(jax.random.fold_in(key, 23), TOKENS, FF, math.sqrt(TOKENS))
    return jnp.clip(values, -16.0, 16.0).astype(jnp.bfloat16)


def draw_weight(key, part):
    keys = jax.random.split(jax.random.fold_in(key, 37), 3)
    values = jax.random.normal(keys[0], (D, FF), jnp.float32)
    row_scale = scales(keys[1], D, 3.0, 10.0) / 4.0
    col_scale = scales(keys[2], FF, 3.0, 10.0) / 4.0
    values = values * row_scale[:, None] * col_scale[None, :] / math.sqrt(D)
    return jnp.clip(values, -1.0, 1.0).astype(jnp.bfloat16)


def steps_of(key, shape, cuts, low, top_value):
    loudness, own = 1.0, jax.random.fold_in(key, 6)
    for axis_at, shards_of in cuts:
        draws = jnp.exp(jax.random.uniform(jax.random.fold_in(own, axis_at), (shards_of,), jnp.float32, low / len(cuts), top_value / len(cuts)))
        loudness = loudness * jnp.repeat(draws, shape[axis_at] // shards_of).reshape([-1 if axis == axis_at else 1 for axis in range(len(shape))])
    return loudness


def setup_inputs(seed: int = 0) -> dict:
    streams_of = jax.random.split(jax.random.key(seed), 6)
    return {
        "activations": draw_activations(jax.random.fold_in(streams_of[5], 71), 0),
        "output_grads": draw_output_grads(jax.random.fold_in(streams_of[5], 71), 0),
        "weight": draw_weight(jax.random.fold_in(streams_of[5], 71), 0),
        "row_moment": jnp.clip(jnp.exp(math.log(0.3) - 3.4011974 * jax.random.uniform(streams_of[3], (D,), jnp.float32) ** steps_of(streams_of[3], (D,), ((0, 4),), -0.2, 0.2)), 0.01, 0.3),
        "col_moment": jnp.clip(jnp.exp(math.log(0.3) - 3.4011974 * jax.random.uniform(streams_of[4], (FF,), jnp.float32) ** steps_of(streams_of[4], (FF,), ((0, 8),), -0.2, 0.2)), 0.01, 0.3),
    }


ADDED_SQUARE = 1e-30
DECAY_RATE = 0.8
CLIP_LIMIT = 1.0
STEP_SIZE = 0.1
MEAN_OFFSET = 1e-06

def reference(activations, output_grads, weight, row_moment, col_moment):
    block_rows = math.gcd(D, 1152)
    block_count = D // block_rows
    left_side = activations.astype(jnp.float32).T.reshape(block_count, block_rows, TOKENS)
    right_side = output_grads.astype(jnp.float32)
    weight_blocks = weight.reshape(block_count, block_rows, FF)

    def grad_block(left_block):
        return jnp.dot(left_block, right_side, preferred_element_type=jnp.float32)

    def first_pass(carry, left_block):
        squared = jnp.square(grad_block(left_block)) + ADDED_SQUARE
        return (carry + lax.optimization_barrier(jnp.sum(squared, axis=0)), lax.optimization_barrier(jnp.sum(squared, axis=1)))
    col_total, row_total = lax.scan(first_pass, jnp.zeros((FF,), jnp.float32), left_side)
    new_row = DECAY_RATE * row_moment + (1.0 - DECAY_RATE) * row_total.reshape(D) / FF
    new_col = DECAY_RATE * col_moment + (1.0 - DECAY_RATE) * col_total / D
    row_mean = jnp.sum(new_row) / D
    row_blocks = new_row.reshape(block_count, block_rows)

    def update_block(left_block, row_block):
        return grad_block(left_block) / jnp.sqrt(row_block[:, None] * new_col[None, :] / row_mean)

    def second_pass(carry, items):
        left_block, row_block, weight_block = items
        update = update_block(left_block, row_block)
        widened = weight_block.astype(jnp.float32)
        return ((carry[0] + jnp.sum(update * update), carry[1] + jnp.sum(widened * widened)), None)
    start = (jnp.zeros((), jnp.float32), jnp.zeros((), jnp.float32))
    (update_total, weight_total), _ = lax.scan(second_pass, start, (left_side, row_blocks, weight_blocks))
    entries = float(D * FF)
    clip_factor = jnp.maximum(1.0, jnp.sqrt(update_total / entries) / CLIP_LIMIT)
    step_scale = STEP_SIZE * jnp.sqrt(weight_total / entries + MEAN_OFFSET)

    def third_pass(items):
        left_block, row_block, weight_block = items
        update = update_block(left_block, row_block)
        return (weight_block.astype(jnp.float32) - step_scale / clip_factor * update).astype(jnp.bfloat16)
    new_weight = lax.map(third_pass, (left_side, row_blocks, weight_blocks)).reshape(D, FF)
    return (new_weight, new_row, new_col)
```

```python
import functools

import jax
import jax.numpy as jnp
from jax import lax
from jax.experimental import pallas as pl
from jax.experimental.pallas import tpu as pltpu
from jax.sharding import PartitionSpec as P

ADDED_SQUARE = 1e-30
DECAY_RATE = 0.8
CLIP_LIMIT = 1.0
STEP_SIZE = 0.1
MEAN_OFFSET = 1e-06
SHARES = (1, 2, 3, 3)


def swap(value, axis, stride):
    size = lax.axis_size(axis)
    return lax.ppermute(value, axis, [(i, i ^ stride) for i in range(size)])


def sum_over(value, axis):
    size = lax.axis_size(axis)
    if size & (size - 1):
        return lax.psum(value, axis)
    stride = 1
    while stride < size:
        if stride * 2 < size:
            near = swap(value, axis, stride)
            far = swap(value, axis, stride * 2)
            both = swap(value, axis, stride * 3)
            value = (value + near) + (far + both)
            stride *= 4
        else:
            value = value + swap(value, axis, stride)
            stride *= 2
    return value


def gather_over(block, axis):
    size = lax.axis_size(axis)
    if size & (size - 1):
        return lax.all_gather(block, axis, axis=0, tiled=True)
    index = lax.axis_index(axis)
    held, depth, stride = block, 0, size // 2
    while stride:
        other = swap(held, axis, stride)
        upper = (index & stride) != 0
        held = jnp.stack([jnp.where(upper, other, held), jnp.where(upper, held, other)], axis=depth)
        depth += 1
        stride //= 2
    return held.reshape((size * block.shape[0],) + block.shape[1:])


def column_cuts(width):
    unit = width // sum(SHARES)
    if unit * sum(SHARES) != width or unit % 128:
        return [(0, width)]
    cuts, start = [], 0
    for share in SHARES:
        cuts.append((start, start + share * unit))
        start += share * unit
    return cuts


def divisor_of(choices, *lengths):
    for choice in choices:
        if all(length % choice == 0 for length in lengths):
            return choice
    return None


def gradient_kernel(tile, left, right, *refs):
    grad, col_sums, row_sums = refs[-3:]
    lanes = row_sums.shape[1]

    @pl.when(pl.program_id(0) == 0)
    def _():
        row_sums[...] = jnp.zeros_like(row_sums)

    col_sums[...] = jnp.zeros_like(col_sums)

    def step(index, carry):
        rows = pl.ds(pl.multiple_of(index * tile, tile), tile)
        value = jnp.dot(left[rows, :], right[...], preferred_element_type=jnp.float32)
        grad[rows, :] = value
        squared = value * value
        width = squared.shape[1]
        col_sums[...] += squared.reshape(tile // 8, 8, width).sum(axis=0)
        if lanes == 1:
            row_sums[rows, :] += squared.sum(axis=1, keepdims=True)
        else:
            groups = [squared[:, k : k + lanes] for k in range(0, width, lanes)]
            row_sums[rows, :] += sum(groups[1:], groups[0])
        return carry

    lax.fori_loop(0, left.shape[0] // tile, step, 0)


def gradient_columns(left, right, whole, start, width):
    rows, depth = left.shape
    size = right.shape[1]
    block = divisor_of((512, 256, 128), start, size) or size
    tile = divisor_of((384, 256, 128, 64, 32, 16, 8), rows)
    lanes = 128 if block % 128 == 0 else 1
    first = start // block
    held = () if whole is None else (whole,)
    return pl.pallas_call(
        functools.partial(gradient_kernel, tile),
        grid=(size // block,),
        in_specs=[
            pl.BlockSpec((rows, depth), lambda j: (0, 0)),
            pl.BlockSpec((depth, block), lambda j: (0, j)),
        ]
        + [pl.BlockSpec(memory_space=pl.ANY)] * len(held),
        out_specs=[
            pl.BlockSpec((rows, block), lambda j: (0, first + j)),
            pl.BlockSpec((8, block), lambda j: (0, j)),
            pl.BlockSpec((rows, lanes), lambda j: (0, 0)),
        ],
        out_shape=[
            jax.ShapeDtypeStruct((rows, width), jnp.float32),
            jax.ShapeDtypeStruct((8, size), jnp.float32),
            jax.ShapeDtypeStruct((rows, lanes), jnp.float32),
        ],
        input_output_aliases={2: 0} if held else {},
        compiler_params=pltpu.CompilerParams(
            dimension_semantics=("arbitrary",), vmem_limit_bytes=40 * 1024 * 1024
        ),
        cost_estimate=pl.CostEstimate(
            flops=2 * rows * depth * size,
            bytes_accessed=rows * size * 4 + depth * size * 2 + rows * depth * 2,
            transcendentals=0,
        ),
    )(left, right, *held)


def on_device(activations, output_grads, weight, row_moment, col_moment):
    tile_rows, tile_cols = weight.shape
    total_rows = tile_rows * lax.axis_size("row")
    total_cols = tile_cols * lax.axis_size("col")
    entries = float(total_rows * total_cols)
    cuts = column_cuts(tile_cols)
    grads = [lax.all_gather(output_grads[:, a:b], "row", axis=0, tiled=True) for a, b in cuts]
    left = gather_over(activations, "col").T
    weight_wide = weight.astype(jnp.float32)
    weight_local = jnp.sum(weight_wide * weight_wide)
    left, weight_local = lax.optimization_barrier((left, weight_local))
    gradient, row_part, col_parts = None, 0.0, [None] * len(cuts)
    for k in reversed(range(len(cuts))):
        gradient, col_sums, row_sums = gradient_columns(left, grads[k], gradient, cuts[k][0], tile_cols)
        row_part = row_part + row_sums
        col_parts[k] = jnp.sum(col_sums, axis=0)
    row_part = jnp.sum(row_part, axis=1)
    col_part = jnp.concatenate(col_parts)
    row_total = sum_over(row_part, "col") + total_cols * ADDED_SQUARE
    col_total = sum_over(col_part, "row") + total_rows * ADDED_SQUARE
    new_row = DECAY_RATE * row_moment + (1.0 - DECAY_RATE) * row_total / total_cols
    new_col = DECAY_RATE * col_moment + (1.0 - DECAY_RATE) * col_total / total_rows
    row_inverse = lax.rsqrt(new_row)
    col_inverse = lax.rsqrt(new_col)
    scaled = gradient * row_inverse[:, None] * col_inverse[None, :]
    ratio_local = jnp.sum(scaled * scaled)
    leader = (lax.axis_index("col") == 0).astype(jnp.float32)
    row_local = leader * jnp.sum(new_row)
    scalars = jnp.stack([row_local, weight_local, ratio_local])
    row_sum, weight_total, ratio_sum = sum_over(sum_over(scalars, "row"), "col")
    row_mean = row_sum / total_rows
    rms_update = jnp.sqrt(row_mean * ratio_sum / entries)
    clip_factor = jnp.maximum(1.0, rms_update / CLIP_LIMIT)
    step_scale = STEP_SIZE * jnp.sqrt(weight_total / entries + MEAN_OFFSET)
    row_factor = row_inverse * (step_scale / clip_factor * jnp.sqrt(row_mean))
    new_weight = (
        weight.astype(jnp.float32) - gradient * row_factor[:, None] * col_inverse[None, :]
    ).astype(jnp.bfloat16)
    return (new_weight, new_row, new_col)


def solution(mesh):
    return jax.shard_map(
        on_device,
        mesh=mesh,
        in_specs=(P("col", "row"), P("row", "col"), P("row", "col"), P("row"), P("col")),
        out_specs=(P("row", "col"), P("row"), P("col")),
        check_vma=False,
    )
```
